512 devices in a mesh: row: 32 (over z_lo, y, core), col: 16 (over z_hi, x).
Axes of the slice: x: 4, y: 8, z: 8 (z_hi: 4, z_lo: 2; z = z_hi * 2 + z_lo), core: 2. Of those that a mesh axis runs over, the one named last changes fastest.
Arguments:
- pixels: float32 [8, 3, 1024, 2048], P(None, None, 'row', 'col'), may hold values from -6 to 6
- factor: float32 [1024, 512], P('row'), may hold values from -6 to 6
Outputs:
- gram: float32 [1024, 1024], P('row', 'col')
- projected: float32 [1024, 512], P('col', 'row')
The draws below stay inside these ranges and needn't reach their ends.
All inputs are finite; a program needn't handle non-finite values.
Results may differ from the reference program's by a relative error of at most 0.000075.
Values sent between devices are 32-bit elements; how exact they have to be, the bound alone decides.
No kernel may reach another device: no remote copies, remote signals or barrier semaphores. Data moves between devices by JAX's collectives and lax.ppermute only.
A program may use at most 64 MiB of HBM per device.

```python
import jax
import jax.numpy as jnp
from jax import lax

H = 1024
W = 2048
C = 3
R = 512
VIEWS = 8


def levels(stream_key, dims, pieces, low, top_value):
    gain, own = 1.0, jax.random.fold_in(stream_key, 6)
    for axis_at, blocks in pieces:
        heights = jnp.exp(jax.random.uniform(jax.random.fold_in(own, axis_at), (blocks,), jnp.float32, low / len(pieces), top_value / len(pieces)))
        gain = gain * jnp.repeat(heights, dims[axis_at] // blocks).reshape([-1 if axis == axis_at else 1 for axis in range(len(dims))])
    return gain


def noise(rng, dims, spread, most, shards=(), kind=jnp.bfloat16):
    values = jax.random.normal(rng, dims, jnp.float32) * spread
    if len(shards) > 0:
        values = levels(rng, dims, shards, -0.22, 0.18) * values
    return jnp.clip(values, min=-most, max=most).astype(kind)


def setup_inputs(seed: int = 0) -> dict:
    streams_of = jax.random.split(jax.random.key(seed), 3)
    pixels = noise(streams_of[0], (VIEWS, C, H, W), 1.0, 6.0, ((2, 32), (3, 16)), jnp.float32)
    factor = noise(streams_of[1], (H, R), 1.0, 6.0, ((0, 32),), jnp.float32)
    return {"pixels": pixels, "factor": factor}


def reference(pixels, factor):
    unfolded = jnp.transpose(pixels, (2, 0, 1, 3)).reshape(H, VIEWS * C * W)
    gram = jnp.dot(unfolded, unfolded.T, precision=lax.Precision.HIGHEST, preferred_element_type=jnp.float32)
    gram = gram / jnp.float32(VIEWS * C * W)
    projected = jnp.dot(gram.T, factor, precision=lax.Precision.HIGHEST, preferred_element_type=jnp.float32)
    return gram, projected
```

```python
import jax
import jax.numpy as jnp
from jax import lax
from jax.experimental import pallas as pl
from jax.experimental.pallas import tpu as pltpu
from jax.sharding import Mesh
from jax.sharding import PartitionSpec as P

AXES = ("zl", "y", "k", "zh", "x")
SIZES = (2, 8, 2, 4, 4)
ROW = ("zl", "y", "k")
COL = ("zh", "x")
PLANES, OWN, LANES = 3, 32, 128
DEPTH = PLANES * LANES
COUNT = 8 * 3 * 2048
NT = (((1,), (1,)), ((), ()))


def call(body, out, scratch=(), operands=1, scalars=0):
    vmem = pl.BlockSpec(memory_space=pltpu.VMEM)
    smem = pl.BlockSpec(memory_space=pltpu.SMEM)
    many = isinstance(out, tuple)
    return pl.pallas_call(
        body,
        out_shape=out,
        in_specs=[smem] * scalars + [vmem] * operands,
        out_specs=tuple(vmem for _ in out) if many else vmem,
        scratch_shapes=list(scratch),
    )


def f32(*shape):
    return jax.ShapeDtypeStruct(shape, jnp.float32)


def pair_body(place, rows, out, high, low):
    for x in range(4):
        for zl in range(2):
            for zh_lo in range(2):
                for k in range(2):
                    at = x * 256 + zl * 128 + zh_lo * 64 + k * 32
                    for p in range(PLANES):
                        v = rows[k, zl * 8 + zh_lo * 4 + x, p * OWN : (p + 1) * OWN, :]
                        h = v.astype(jnp.bfloat16)
                        high[at : at + OWN, p * LANES : (p + 1) * LANES] = h
                        low[at : at + OWN, p * LANES : (p + 1) * LANES] = (v - h.astype(jnp.float32)).astype(jnp.bfloat16)
    own = place[0] * 128 + place[1] * 32

    def own_rows(ref):
        return jnp.concatenate([ref[pl.ds(pl.multiple_of(own + (y % 4) * 256 + (y // 4) * 64, 32), OWN), :] for y in range(8)], axis=0)

    own_high, own_low = own_rows(high), own_rows(low)
    for x in range(4):
        h, l = high[x * 256 : (x + 1) * 256, :], low[x * 256 : (x + 1) * 256, :]
        g = lax.dot_general(own_high, l, NT, preferred_element_type=jnp.float32)
        g += lax.dot_general(own_low, h, NT, preferred_element_type=jnp.float32)
        g += lax.dot_general(own_high, h, NT, preferred_element_type=jnp.float32)
        out[x, 0] = g[:, :LANES]
        out[x, 1] = g[:, LANES:]


def fold_body(parts, out):
    left = lax.broadcasted_iota(jnp.int32, (16, LANES), 1) < 64
    for zh in range(2):
        for y in range(8):
            v = parts[0, zh, y * OWN : (y + 1) * OWN, :]
            for x in range(1, 4):
                v += parts[x, zh, y * OWN : (y + 1) * OWN, :]
            a, b = v[:16], v[16:]
            out[zh * 2, y] = jnp.where(left, a, pltpu.roll(b, 64, 1))
            out[zh * 2 + 1, y] = jnp.where(left, pltpu.roll(a, 64, 1), b)


def term_body(parts, factor, gram, term):
    g = jnp.sum(parts[...], axis=0) / COUNT
    block = jnp.concatenate([g[:, :64], g[:, 64:]], axis=0)
    gram[...] = block
    t = lax.dot_general(
        factor[...], block, (((0,), (0,)), ((), ())), precision=lax.Precision.HIGHEST, preferred_element_type=jnp.float32
    )
    for r in range(32):
        term[r] = jnp.concatenate([t[r * 16 : r * 16 + 8], t[r * 16 + 8 : r * 16 + 16]], axis=1)


def close_body(parts, out):
    v = jnp.sum(parts[...], axis=0)
    out[...] = jnp.concatenate([v[:, :64], v[:, 64:]], axis=0)


def swap(array, axes):
    return lax.all_to_all(array, axes, 0, 0, tiled=True)


def shards(pixels, factor):
    place = jnp.stack([lax.axis_index("zl"), lax.axis_index("k")]).astype(jnp.int32)
    own = pixels.reshape(8, PLANES * OWN, LANES)
    rows = swap(jnp.broadcast_to(own[None], (2, *own.shape)).reshape(16, *own.shape[1:]), ("zl", "y"))
    rows = swap(jnp.broadcast_to(rows[None], (2, *rows.shape)), "k")
    wide = pltpu.VMEM((1024, DEPTH), jnp.bfloat16)
    partial_gram = call(pair_body, f32(4, 2, 256, LANES), (wide, wide), 1, 1)(place, rows)
    partial_gram = swap(partial_gram.reshape(4, 512, LANES), "x").reshape(4, 2, 256, LANES)
    folded = call(fold_body, f32(4, 8, 16, LANES))(partial_gram)
    folded = swap(folded.reshape(32, 16, LANES), ("zh", "y"))
    gram, term = call(term_body, (f32(32, 64), f32(32, 8, LANES)), (), 2)(folded, factor)
    projected = call(close_body, f32(16, 64))(swap(term, ROW))
    return gram, projected.T


def solution(mesh):
    split = Mesh(mesh.devices.reshape(SIZES), AXES)
    in_specs = (P(None, None, ROW, COL), P(ROW, None))
    out_specs = (P(ROW, COL), P(COL, ROW))
    return jax.shard_map(shards, mesh=split, in_specs=in_specs, out_specs=out_specs, check_vma=False)
```

```python
import jax
import jax.numpy as jnp
from jax import lax
from jax.experimental import pallas as pl
from jax.experimental.pallas import tpu as pltpu
from jax.sharding import Mesh
from jax.sharding import PartitionSpec as P

AXES = ("zl", "y", "k", "zh", "x")
SIZES = (2, 8, 2, 4, 4)
ROW = ("zl", "y", "k")
COL = ("zh", "x")
PLANES, OWN, LANES = 3, 32, 128
DEPTH = PLANES * LANES
COUNT = 8 * 3 * 2048
NT = (((1,), (1,)), ((), ()))


def call(body, out, scratch=(), operands=1):
    vmem = pl.BlockSpec(memory_space=pltpu.VMEM)
    many = isinstance(out, tuple)
    kernel = pl.pallas_call(
        body,
        out_shape=out,
        in_specs=[vmem] * operands,
        out_specs=tuple(vmem for _ in out) if many else vmem,
        scratch_shapes=list(scratch),
    )
    return lambda *arrays: kernel(*(pltpu.with_memory_space_constraint(a, pltpu.VMEM) for a in arrays))


def f32(*shape):
    return pltpu.VMEM(shape, jnp.float32)


def result(*shape):
    return jax.ShapeDtypeStruct(shape, jnp.float32)


def pair_body(rows, out, high, low):
    for x in range(4):
        for zl in range(2):
            for zh_lo in range(2):
                for k in range(2):
                    at = x * 256 + zl * 128 + zh_lo * 64 + k * 32
                    for p in range(PLANES):
                        v = rows[k, zl * 8 + zh_lo * 4 + x, p * OWN : (p + 1) * OWN, :]
                        h = v.astype(jnp.bfloat16)
                        high[at : at + OWN, p * LANES : (p + 1) * LANES] = h
                        low[at : at + OWN, p * LANES : (p + 1) * LANES] = (v - h.astype(jnp.float32)).astype(jnp.bfloat16)
    own = lax.axis_index("zl") * 128 + lax.axis_index("k") * 32

    def own_rows(ref):
        return jnp.concatenate([ref[pl.ds(pl.multiple_of(own + (y % 4) * 256 + (y // 4) * 64, 32), OWN), :] for y in range(8)], axis=0)

    own_high, own_low = own_rows(high), own_rows(low)
    for x in range(4):
        h, l = high[x * 256 : (x + 1) * 256, :], low[x * 256 : (x + 1) * 256, :]
        g = lax.dot_general(own_high, l, NT, preferred_element_type=jnp.float32)
        g += lax.dot_general(own_low, h, NT, preferred_element_type=jnp.float32)
        g += lax.dot_general(own_high, h, NT, preferred_element_type=jnp.float32)
        out[x, 0] = g[:, :LANES]
        out[x, 1] = g[:, LANES:]


def fold_body(parts, out):
    left = lax.broadcasted_iota(jnp.int32, (16, LANES), 1) < 64
    for zh in range(2):
        for y in range(8):
            v = parts[0, zh, y * OWN : (y + 1) * OWN, :]
            for x in range(1, 4):
                v += parts[x, zh, y * OWN : (y + 1) * OWN, :]
            a, b = v[:16], v[16:]
            out[zh * 2, y] = jnp.where(left, a, pltpu.roll(b, 64, 1))
            out[zh * 2 + 1, y] = jnp.where(left, pltpu.roll(a, 64, 1), b)


def term_body(parts, factor, gram, term):
    g = jnp.sum(parts[...], axis=0) / COUNT
    block = jnp.concatenate([g[:, :64], g[:, 64:]], axis=0)
    gram[...] = block
    t = lax.dot_general(
        factor[...], block, (((0,), (0,)), ((), ())), precision=lax.Precision.HIGHEST, preferred_element_type=jnp.float32
    )
    for r in range(32):
        term[r] = jnp.concatenate([t[r * 16 : r * 16 + 8], t[r * 16 + 8 : r * 16 + 16]], axis=1)


def close_body(parts, out):
    v = jnp.sum(parts[...], axis=0)
    out[...] = jnp.concatenate([v[:, :64], v[:, 64:]], axis=0)


def swap(array, axes):
    return lax.all_to_all(array, axes, 0, 0, tiled=True)


def both(array, axis):
    return swap(jnp.broadcast_to(array[None], (2, *array.shape)), axis)


def shards(pixels, factor):
    own = pixels.reshape(8, PLANES * OWN, LANES)
    rows = both(swap(own, "y"), "zl")
    rows = both(rows.reshape(16, *own.shape[1:]), "k")
    wide = pltpu.VMEM((1024, DEPTH), jnp.bfloat16)
    partial_gram = call(pair_body, f32(4, 2, 256, LANES), (wide, wide))(rows)
    partial_gram = swap(partial_gram.reshape(4, 512, LANES), "x").reshape(4, 2, 256, LANES)
    folded = call(fold_body, f32(4, 8, 16, LANES))(partial_gram)
    folded = swap(folded.reshape(32, 16, LANES), ("zh", "y"))
    gram, term = call(term_body, (result(32, 64), f32(32, 8, LANES)), (), 2)(folded, factor)
    projected = call(close_body, result(16, 64))(swap(term, ROW))
    return gram, projected.T


def solution(mesh):
    split = Mesh(mesh.devices.reshape(SIZES), AXES)
    in_specs = (P(None, None, ROW, COL), P(ROW, None))
    out_specs = (P(ROW, COL), P(COL, ROW))
    return jax.shard_map(shards, mesh=split, in_specs=in_specs, out_specs=out_specs, check_vma=False)
```

```python
import jax
import jax.numpy as jnp
from jax import lax
from jax.experimental import pallas as pl
from jax.experimental.pallas import tpu as pltpu
from jax.sharding import Mesh
from jax.sharding import PartitionSpec as P

AXES = ("zl", "yh", "yl", "k", "zh", "x")
SIZES = (2, 4, 2, 2, 4, 4)
ROW = ("zl", "yh", "yl", "k")
COL = ("zh", "x")
PLANES, OWN, LANES = 3, 32, 128
DEPTH = PLANES * LANES
COUNT = 8 * 3 * 2048
NT = (((1,), (1,)), ((), ()))


def call(body, out, scratch=(), operands=1):
    vmem = pl.BlockSpec(memory_space=pltpu.VMEM)
    many = isinstance(out, tuple)
    kernel = pl.pallas_call(
        body,
        out_shape=out,
        in_specs=[vmem] * operands,
        out_specs=tuple(vmem for _ in out) if many else vmem,
        scratch_shapes=list(scratch),
    )
    return lambda *arrays: kernel(*(pltpu.with_memory_space_constraint(a, pltpu.VMEM) for a in arrays))


def f32(*shape):
    return pltpu.VMEM(shape, jnp.float32)


def result(*shape):
    return jax.ShapeDtypeStruct(shape, jnp.float32)


def pair_body(rows, out, high, low):
    for x in range(4):
        for zl in range(2):
            for zh_lo in range(2):
                for k in range(2):
                    at = x * 256 + zl * 128 + zh_lo * 64 + k * 32
                    for p in range(PLANES):
                        v = rows[k, zl * 8 + zh_lo * 4 + x, p * OWN : (p + 1) * OWN, :]
                        h = v.astype(jnp.bfloat16)
                        high[at : at + OWN, p * LANES : (p + 1) * LANES] = h
                        low[at : at + OWN, p * LANES : (p + 1) * LANES] = (v - h.astype(jnp.float32)).astype(jnp.bfloat16)
    own = lax.axis_index("zl") * 128 + lax.axis_index("k") * 32

    def own_rows(ref):
        order = [yh * 2 + yl for yl in range(2) for yh in range(4)]
        return jnp.concatenate([ref[pl.ds(pl.multiple_of(own + (y % 4) * 256 + (y // 4) * 64, 32), OWN), :] for y in order], axis=0)

    own_high, own_low = own_rows(high), own_rows(low)
    for x in range(4):
        h, l = high[x * 256 : (x + 1) * 256, :], low[x * 256 : (x + 1) * 256, :]
        g = lax.dot_general(own_high, l, NT, preferred_element_type=jnp.float32)
        g += lax.dot_general(own_low, h, NT, preferred_element_type=jnp.float32)
        g += lax.dot_general(own_high, h, NT, preferred_element_type=jnp.float32)
        for yl in range(2):
            for zl in range(2):
                out[x, yl, zl] = g[yl * 128 : (yl + 1) * 128, zl * LANES : (zl + 1) * LANES]


def fold_body(parts, out):
    left = lax.broadcasted_iota(jnp.int32, (16, LANES), 1) < 64
    for zh in range(2):
        for y in range(4):
            v = parts[0, zh, y * OWN : (y + 1) * OWN, :]
            for src in range(1, 8):
                v += parts[src, zh, y * OWN : (y + 1) * OWN, :]
            a, b = v[:16], v[16:]
            out[zh * 2, y] = jnp.where(left, a, pltpu.roll(b, 64, 1))
            out[zh * 2 + 1, y] = jnp.where(left, pltpu.roll(a, 64, 1), b)


def term_body(parts, factor, gram, term):
    g = jnp.sum(parts[...], axis=0) / COUNT
    block = jnp.concatenate([g[:, :64], g[:, 64:]], axis=0)
    gram[...] = block
    t = lax.dot_general(
        factor[...], block, (((0,), (0,)), ((), ())), precision=lax.Precision.HIGHEST, preferred_element_type=jnp.float32
    )
    for r in range(32):
        term[r] = jnp.concatenate([t[r * 16 : r * 16 + 8], t[r * 16 + 8 : r * 16 + 16]], axis=1)


def close_body(parts, out):
    v = jnp.sum(parts[...], axis=0)
    out[...] = jnp.concatenate([v[:, :64], v[:, 64:]], axis=0)


def swap(array, axes):
    return lax.all_to_all(array, axes, 0, 0, tiled=True)


def both(array, axis):
    return swap(jnp.broadcast_to(array[None], (2, *array.shape)), axis)


def shards(pixels, factor):
    own = pixels.reshape(8, PLANES * OWN, LANES)
    rows = swap(jnp.concatenate([own, own]), ("zl", "yh", "yl"))
    rows = both(rows, "k")
    wide = pltpu.VMEM((1024, DEPTH), jnp.bfloat16)
    partial_gram = call(pair_body, f32(4, 2, 2, 128, LANES), (wide, wide))(rows)
    partial_gram = swap(partial_gram.reshape(8, 256, LANES), ("x", "yl"))
    folded = call(fold_body, f32(4, 4, 16, LANES))(partial_gram.reshape(8, 2, 128, LANES))
    folded = swap(folded.reshape(16, 16, LANES), ("zh", "yh"))
    gram, term = call(term_body, (result(32, 64), f32(32, 8, LANES)), (), 2)(folded, factor)
    projected = call(close_body, result(16, 64))(swap(term, ROW))
    return gram, projected.T


def solution(mesh):
    split = Mesh(mesh.devices.reshape(SIZES), AXES)
    in_specs = (P(None, None, ROW, COL), P(ROW, None))
    out_specs = (P(ROW, COL), P(COL, ROW))
    return jax.shard_map(shards, mesh=split, in_specs=in_specs, out_specs=out_specs, check_vma=False)
```

```python
import jax
import jax.numpy as jnp
from jax import lax
from jax.experimental import pallas as pl
from jax.experimental.pallas import tpu as pltpu
from jax.sharding import Mesh
from jax.sharding import PartitionSpec as P

AXES = ("zl", "yo", "ya", "yb", "k", "zh", "x")
SIZES = (2, 2, 2, 2, 2, 4, 4)
ROW = ("zl", "yo", "ya", "yb", "k")
COL = ("zh", "x")
PLANES, OWN, LANES = 3, 32, 128
DEPTH = PLANES * LANES
COUNT = 8 * 3 * 2048
NT = (((1,), (1,)), ((), ()))


def call(body, out, scratch=(), operands=1):
    vmem = pl.BlockSpec(memory_space=pltpu.VMEM)
    many = isinstance(out, tuple)
    kernel = pl.pallas_call(
        body,
        out_shape=out,
        in_specs=[vmem] * operands,
        out_specs=tuple(vmem for _ in out) if many else vmem,
        scratch_shapes=list(scratch),
    )
    return lambda *arrays: kernel(*(pltpu.with_memory_space_constraint(a, pltpu.VMEM) for a in arrays))


def f32(*shape):
    return pltpu.VMEM(shape, jnp.float32)


def result(*shape):
    return jax.ShapeDtypeStruct(shape, jnp.float32)


def pair_body(rows, out, high, low):
    for x in range(4):
        for zl in range(2):
            for zh_lo in range(2):
                for k in range(2):
                    at = x * 256 + zl * 128 + zh_lo * 64 + k * 32
                    for p in range(PLANES):
                        v = rows[k, zl * 8 + zh_lo * 4 + x, p * OWN : (p + 1) * OWN, :]
                        h = v.astype(jnp.bfloat16)
                        high[at : at + OWN, p * LANES : (p + 1) * LANES] = h
                        low[at : at + OWN, p * LANES : (p + 1) * LANES] = (v - h.astype(jnp.float32)).astype(jnp.bfloat16)
    own = lax.axis_index("yo") * 64 + lax.axis_index("k") * 32

    def own_rows(ref):
        order = [(ya * 2 + yb) * 256 + zl * 128 for yb in range(2) for zl in range(2) for ya in range(2)]
        return jnp.concatenate([ref[pl.ds(pl.multiple_of(own + at, 32), OWN), :] for at in order], axis=0)

    own_high, own_low = own_rows(high), own_rows(low)
    for x in range(4):
        h, l = high[x * 256 : (x + 1) * 256, :], low[x * 256 : (x + 1) * 256, :]
        g = lax.dot_general(own_high, l, NT, preferred_element_type=jnp.float32)
        g += lax.dot_general(own_low, h, NT, preferred_element_type=jnp.float32)
        g += lax.dot_general(own_high, h, NT, preferred_element_type=jnp.float32)
        for yb in range(2):
            for zh in range(2):
                out[x, yb, zh] = g[yb * 128 : (yb + 1) * 128, zh * LANES : (zh + 1) * LANES]


def fold_body(parts, out):
    left = lax.broadcasted_iota(jnp.int32, (16, LANES), 1) < 64
    for zh in range(2):
        for zl in range(2):
            for ya in range(2):
                at = (zl * 2 + ya) * OWN
                v = parts[0, zh, at : at + OWN, :]
                for src in range(1, 8):
                    v += parts[src, zh, at : at + OWN, :]
                a, b = v[:16], v[16:]
                out[zl, zh * 2, ya] = jnp.where(left, a, pltpu.roll(b, 64, 1))
                out[zl, zh * 2 + 1, ya] = jnp.where(left, pltpu.roll(a, 64, 1), b)


def term_body(parts, factor, gram, term):
    g = jnp.sum(parts[...], axis=0) / COUNT
    block = jnp.concatenate([g[:, :64], g[:, 64:]], axis=0)
    gram[...] = block
    t = lax.dot_general(
        factor[...], block, (((0,), (0,)), ((), ())), precision=lax.Precision.HIGHEST, preferred_element_type=jnp.float32
    )
    for r in range(32):
        term[r] = jnp.concatenate([t[r * 16 : r * 16 + 8], t[r * 16 + 8 : r * 16 + 16]], axis=1)


def close_body(parts, out):
    v = jnp.sum(parts[...], axis=0)
    out[...] = jnp.concatenate([v[:, :64], v[:, 64:]], axis=0)


def swap(array, axes):
    return lax.all_to_all(array, axes, 0, 0, tiled=True)


def both(array, axis):
    return swap(jnp.broadcast_to(array[None], (2, *array.shape)), axis)


def shards(pixels, factor):
    own = pixels.reshape(2, 1, 4, PLANES * OWN, LANES)
    rows = swap(jnp.concatenate([own, own], axis=1).reshape(16, PLANES * OWN, LANES), ("zl", "yo", "ya", "yb"))
    rows = both(rows, "k")
    wide = pltpu.VMEM((1024, DEPTH), jnp.bfloat16)
    partial_gram = call(pair_body, f32(4, 2, 2, 128, LANES), (wide, wide))(rows)
    partial_gram = swap(partial_gram.reshape(8, 256, LANES), ("x", "yb"))
    folded = call(fold_body, f32(2, 4, 2, 16, LANES))(partial_gram.reshape(8, 2, 128, LANES))
    folded = swap(folded.reshape(16, 16, LANES), ("zl", "zh", "ya"))
    gram, term = call(term_body, (result(32, 64), f32(32, 8, LANES)), (), 2)(folded, factor)
    projected = call(close_body, result(16, 64))(swap(term, ROW))
    return gram, projected.T


def solution(mesh):
    split = Mesh(mesh.devices.reshape(SIZES), AXES)
    in_specs = (P(None, None, ROW, COL), P(ROW, None))
    out_specs = (P(ROW, COL), P(COL, ROW))
    return jax.shard_map(shards, mesh=split, in_specs=in_specs, out_specs=out_specs, check_vma=False)
```

```python
import jax
import jax.numpy as jnp
from jax import lax
from jax.experimental import pallas as pl
from jax.experimental.pallas import tpu as pltpu
from jax.sharding import Mesh
from jax.sharding import PartitionSpec as P

AXES = ("zl", "yo", "ya", "yb", "k", "zh", "x")
SIZES = (2, 2, 2, 2, 2, 4, 4)
ROW = ("zl", "yo", "ya", "yb", "k")
COL = ("zh", "x")
PLANES, OWN, LANES = 3, 32, 128
DEPTH = PLANES * LANES
COUNT = 8 * 3 * 2048
NT = (((1,), (1,)), ((), ()))


def call(body, out, scratch=(), operands=1):
    vmem = pl.BlockSpec(memory_space=pltpu.VMEM)
    many = isinstance(out, tuple)
    kernel = pl.pallas_call(
        body,
        out_shape=out,
        in_specs=[vmem] * operands,
        out_specs=tuple(vmem for _ in out) if many else vmem,
        scratch_shapes=list(scratch),
    )
    return lambda *arrays: kernel(*(pltpu.with_memory_space_constraint(a, pltpu.VMEM) for a in arrays))


def f32(*shape):
    return pltpu.VMEM(shape, jnp.float32)


def result(*shape):
    return jax.ShapeDtypeStruct(shape, jnp.float32)


def pair_body(rows, out, high, low):
    for x in range(4):
        for zl in range(2):
            for zh_lo in range(2):
                for k in range(2):
                    at = x * 256 + zl * 128 + zh_lo * 64 + k * 32
                    for p in range(PLANES):
                        v = rows[k, zh_lo * 8 + zl * 4 + x, p * OWN : (p + 1) * OWN, :]
                        h = v.astype(jnp.bfloat16)
                        high[at : at + OWN, p * LANES : (p + 1) * LANES] = h
                        low[at : at + OWN, p * LANES : (p + 1) * LANES] = (v - h.astype(jnp.float32)).astype(jnp.bfloat16)
    own = lax.axis_index("yo") * 64 + lax.axis_index("k") * 32

    def own_rows(ref):
        order = [(ya * 2 + yb) * 256 + zl * 128 for yb in range(2) for zl in range(2) for ya in range(2)]
        return jnp.concatenate([ref[pl.ds(pl.multiple_of(own + at, 32), OWN), :] for at in order], axis=0)

    own_high, own_low = own_rows(high), own_rows(low)
    for x in range(4):
        h, l = high[x * 256 : (x + 1) * 256, :], low[x * 256 : (x + 1) * 256, :]
        g = lax.dot_general(own_high, l, NT, preferred_element_type=jnp.float32)
        g += lax.dot_general(own_low, h, NT, preferred_element_type=jnp.float32)
        g += lax.dot_general(own_high, h, NT, preferred_element_type=jnp.float32)
        for at in range(4):
            for zh in range(2):
                out[x, at, zh] = g[at * 64 : (at + 1) * 64, zh * LANES : (zh + 1) * LANES]


def fold_body(parts, out):
    left = lax.broadcasted_iota(jnp.int32, (16, LANES), 1) < 64
    for zh in range(2):
        for y in range(2):
            v = parts[0, zh, y * OWN : (y + 1) * OWN, :]
            for src in range(1, 16):
                v += parts[src, zh, y * OWN : (y + 1) * OWN, :]
            a, b = v[:16], v[16:]
            out[zh * 2, y] = jnp.where(left, a, pltpu.roll(b, 64, 1))
            out[zh * 2 + 1, y] = jnp.where(left, pltpu.roll(a, 64, 1), b)


def term_body(parts, factor, gram, term):
    g = jnp.sum(parts[...], axis=0) / COUNT
    block = jnp.concatenate([g[:, :64], g[:, 64:]], axis=0)
    gram[...] = block
    t = lax.dot_general(
        factor[...], block, (((0,), (0,)), ((), ())), precision=lax.Precision.HIGHEST, preferred_element_type=jnp.float32
    )
    for r in range(32):
        term[r] = jnp.concatenate([t[r * 16 : r * 16 + 8], t[r * 16 + 8 : r * 16 + 16]], axis=1)


def close_body(parts, block, gram, out):
    gram[...] = block[...]
    v = jnp.sum(parts[...], axis=0)
    out[...] = jnp.concatenate([v[:, :64], v[:, 64:]], axis=0)


def swap(array, axes):
    return lax.all_to_all(array, axes, 0, 0, tiled=True)


def both(array, axis):
    return swap(jnp.broadcast_to(array[None], (2, *array.shape)), axis)


def shards(pixels, factor):
    own = pixels.reshape(8, PLANES * OWN, LANES)
    rows = swap(jnp.concatenate([own, own]), ("yo", "zl", "ya", "yb"))
    rows = both(rows, "k")
    wide = pltpu.VMEM((1024, DEPTH), jnp.bfloat16)
    partial_gram = call(pair_body, f32(4, 4, 2, 64, LANES), (wide, wide))(rows)
    partial_gram = swap(partial_gram.reshape(16, 128, LANES), ("x", "yb", "zl"))
    folded = call(fold_body, f32(4, 2, 16, LANES))(partial_gram.reshape(16, 2, 64, LANES))
    folded = swap(folded.reshape(8, 16, LANES), ("zh", "ya"))
    block, term = call(term_body, (f32(32, 64), f32(32, 8, LANES)), (), 2)(folded, factor)
    gram, projected = call(close_body, (result(32, 64), result(16, 64)), (), 2)(swap(term, ROW), block)
    return gram, projected.T


def solution(mesh):
    split = Mesh(mesh.devices.reshape(SIZES), AXES)
    in_specs = (P(None, None, ROW, COL), P(ROW, None))
    out_specs = (P(ROW, COL), P(COL, ROW))
    return jax.shard_map(shards, mesh=split, in_specs=in_specs, out_specs=out_specs, check_vma=False)
```

```python
import jax
import jax.numpy as jnp
from jax import lax
from jax.experimental import pallas as pl
from jax.experimental.pallas import tpu as pltpu
from jax.sharding import Mesh
from jax.sharding import PartitionSpec as P

AXES = ("zl", "yo", "ya", "yb", "k", "zh", "x")
SIZES = (2, 2, 2, 2, 2, 4, 4)
ROW = ("zl", "yo", "ya", "yb", "k")
COL = ("zh", "x")
PLANES, OWN, LANES = 3, 32, 128
DEPTH = PLANES * LANES
COUNT = 8 * 3 * 2048
NT = (((1,), (1,)), ((), ()))


def call(body, out, scratch=(), operands=1):
    vmem = pl.BlockSpec(memory_space=pltpu.VMEM)
    many = isinstance(out, tuple)
    kernel = pl.pallas_call(
        body,
        out_shape=out,
        in_specs=[vmem] * operands,
        out_specs=tuple(vmem for _ in out) if many else vmem,
        scratch_shapes=list(scratch),
    )
    return lambda *arrays: kernel(*(pltpu.with_memory_space_constraint(a, pltpu.VMEM) for a in arrays))


def f32(*shape):
    return pltpu.VMEM(shape, jnp.float32)


def result(*shape):
    return jax.ShapeDtypeStruct(shape, jnp.float32)


def pair_body(mine, theirs, out, high, low):
    core = lax.axis_index("k")
    for x in range(4):
        for zl in range(2):
            for zh_lo in range(2):
                for rows, k in ((mine, core), (theirs, 1 - core)):
                    at = pl.multiple_of(x * 256 + zl * 128 + zh_lo * 64 + k * 32, 32)
                    for p in range(PLANES):
                        v = rows[zh_lo * 8 + zl * 4 + x, p * OWN : (p + 1) * OWN, :]
                        h = v.astype(jnp.bfloat16)
                        high[pl.ds(at, OWN), p * LANES : (p + 1) * LANES] = h
                        low[pl.ds(at, OWN), p * LANES : (p + 1) * LANES] = (v - h.astype(jnp.float32)).astype(jnp.bfloat16)
    own = lax.axis_index("yo") * 64 + core * 32

    def own_rows(ref):
        order = [(ya * 2 + yb) * 256 + zl * 128 for yb in range(2) for zl in range(2) for ya in range(2)]
        return jnp.concatenate([ref[pl.ds(pl.multiple_of(own + at, 32), OWN), :] for at in order], axis=0)

    own_high, own_low = own_rows(high), own_rows(low)
    for x in range(4):
        h, l = high[x * 256 : (x + 1) * 256, :], low[x * 256 : (x + 1) * 256, :]
        g = lax.dot_general(own_high, l, NT, preferred_element_type=jnp.float32)
        g += lax.dot_general(own_low, h, NT, preferred_element_type=jnp.float32)
        g += lax.dot_general(own_high, h, NT, preferred_element_type=jnp.float32)
        for at in range(4):
            for zh in range(2):
                out[x, at, zh] = g[at * 64 : (at + 1) * 64, zh * LANES : (zh + 1) * LANES]


def fold_body(parts, out):
    left = lax.broadcasted_iota(jnp.int32, (16, LANES), 1) < 64
    for zh in range(2):
        for y in range(2):
            v = parts[0, zh, y * OWN : (y + 1) * OWN, :]
            for src in range(1, 16):
                v += parts[src, zh, y * OWN : (y + 1) * OWN, :]
            a, b = v[:16], v[16:]
            out[zh * 2, y] = jnp.where(left, a, pltpu.roll(b, 64, 1))
            out[zh * 2 + 1, y] = jnp.where(left, pltpu.roll(a, 64, 1), b)


def term_body(parts, factor, gram, term):
    g = jnp.sum(parts[...], axis=0) / COUNT
    block = jnp.concatenate([g[:, :64], g[:, 64:]], axis=0)
    gram[...] = block
    t = lax.dot_general(
        factor[...], block, (((0,), (0,)), ((), ())), precision=lax.Precision.HIGHEST, preferred_element_type=jnp.float32
    )
    for r in range(32):
        term[r] = jnp.concatenate([t[r * 16 : r * 16 + 8], t[r * 16 + 8 : r * 16 + 16]], axis=1)


def close_body(parts, block, gram, out):
    gram[...] = block[...]
    v = jnp.sum(parts[...], axis=0)
    out[...] = jnp.concatenate([v[:, :64], v[:, 64:]], axis=0)


def swap(array, axes):
    return lax.all_to_all(array, axes, 0, 0, tiled=True)


def shards(pixels, factor):
    own = pixels.reshape(8, PLANES * OWN, LANES)
    rows = swap(jnp.concatenate([own, own]), ("yo", "zl", "ya", "yb"))
    theirs = lax.ppermute(rows, "k", [(0, 1), (1, 0)])
    wide = pltpu.VMEM((1024, DEPTH), jnp.bfloat16)
    partial_gram = call(pair_body, f32(4, 4, 2, 64, LANES), (wide, wide), 2)(rows, theirs)
    partial_gram = swap(partial_gram.reshape(16, 128, LANES), ("x", "yb", "zl"))
    folded = call(fold_body, f32(4, 2, 16, LANES))(partial_gram.reshape(16, 2, 64, LANES))
    folded = swap(folded.reshape(8, 16, LANES), ("zh", "ya"))
    block, term = call(term_body, (f32(32, 64), f32(32, 8, LANES)), (), 2)(folded, factor)
    gram, projected = call(close_body, (result(32, 64), result(16, 64)), (), 2)(swap(term, ROW), block)
    return gram, projected.T


def solution(mesh):
    split = Mesh(mesh.devices.reshape(SIZES), AXES)
    in_specs = (P(None, None, ROW, COL), P(ROW, None))
    out_specs = (P(ROW, COL), P(COL, ROW))
    return jax.shard_map(shards, mesh=split, in_specs=in_specs, out_specs=out_specs, check_vma=False)
```

```python
import jax
import jax.numpy as jnp
from jax import lax
from jax.experimental import pallas as pl
from jax.experimental.pallas import tpu as pltpu
from jax.sharding import Mesh
from jax.sharding import PartitionSpec as P

AXES = ("zl", "yo", "ya", "yb", "k", "zh", "x")
SIZES = (2, 2, 2, 2, 2, 4, 4)
ROW = ("zl", "yo", "ya", "yb", "k")
COL = ("zh", "x")
PLANES, OWN, LANES = 3, 32, 128
DEPTH = PLANES * LANES
COUNT = 8 * 3 * 2048
NT = (((1,), (1,)), ((), ()))


def call(body, out, scratch=(), operands=1):
    vmem = pl.BlockSpec(memory_space=pltpu.VMEM)
    many = isinstance(out, tuple)
    kernel = pl.pallas_call(
        body,
        out_shape=out,
        in_specs=[vmem] * operands,
        out_specs=tuple(vmem for _ in out) if many else vmem,
        scratch_shapes=list(scratch),
    )
    return lambda *arrays: kernel(*(pltpu.with_memory_space_constraint(a, pltpu.VMEM) for a in arrays))


def f32(*shape):
    return pltpu.VMEM(shape, jnp.float32)


def result(*shape):
    return jax.ShapeDtypeStruct(shape, jnp.float32)


def twice_body(pixels, out, done):
    copies = [pltpu.make_async_copy(pixels.at[pl.ds(2 * i, 2)], out.at[pl.ds(2 * i, 2)], done.at[i]) for i in range(4)]
    for copy in copies:
        copy.start()
    for i, copy in enumerate(copies):
        copy.wait()
        out[8 + 2 * i : 10 + 2 * i] = out[2 * i : 2 * i + 2]


def twice(pixels):
    return pl.pallas_call(
        twice_body,
        out_shape=pltpu.VMEM((16, *pixels.shape[1:]), jnp.float32),
        in_specs=[pl.BlockSpec(memory_space=pltpu.HBM)],
        out_specs=pl.BlockSpec(memory_space=pltpu.VMEM),
        scratch_shapes=[pltpu.SemaphoreType.DMA((4,))],
    )(pixels)


def pair_body(mine, theirs, out, high, low):
    core = lax.axis_index("k")
    for x in range(4):
        for zl in range(2):
            for zh_lo in range(2):
                for rows, k in ((mine, core), (theirs, 1 - core)):
                    at = pl.multiple_of(x * 256 + zl * 128 + zh_lo * 64 + k * 32, 32)
                    for p in range(PLANES):
                        v = rows[zh_lo * 8 + zl * 4 + x, p * OWN : (p + 1) * OWN, :]
                        h = v.astype(jnp.bfloat16)
                        high[pl.ds(at, OWN), p * LANES : (p + 1) * LANES] = h
                        low[pl.ds(at, OWN), p * LANES : (p + 1) * LANES] = (v - h.astype(jnp.float32)).astype(jnp.bfloat16)
    own = lax.axis_index("yo") * 64 + core * 32

    def own_rows(ref):
        order = [(ya * 2 + yb) * 256 + zl * 128 for yb in range(2) for zl in range(2) for ya in range(2)]
        return jnp.concatenate([ref[pl.ds(pl.multiple_of(own + at, 32), OWN), :] for at in order], axis=0)

    own_high, own_low = own_rows(high), own_rows(low)
    for x in range(4):
        h, l = high[x * 256 : (x + 1) * 256, :], low[x * 256 : (x + 1) * 256, :]
        g = lax.dot_general(own_high, l, NT, preferred_element_type=jnp.float32)
        g += lax.dot_general(own_low, h, NT, preferred_element_type=jnp.float32)
        g += lax.dot_general(own_high, h, NT, preferred_element_type=jnp.float32)
        for at in range(4):
            for zh in range(2):
                out[x, at, zh] = g[at * 64 : (at + 1) * 64, zh * LANES : (zh + 1) * LANES]


def fold_body(parts, out):
    left = lax.broadcasted_iota(jnp.int32, (16, LANES), 1) < 64
    for zh in range(2):
        for y in range(2):
            v = parts[0, zh, y * OWN : (y + 1) * OWN, :]
            for src in range(1, 16):
                v += parts[src, zh, y * OWN : (y + 1) * OWN, :]
            a, b = v[:16], v[16:]
            out[zh * 2, y] = jnp.where(left, a, pltpu.roll(b, 64, 1))
            out[zh * 2 + 1, y] = jnp.where(left, pltpu.roll(a, 64, 1), b)


def term_body(parts, factor, gram, term):
    g = jnp.sum(parts[...], axis=0) / COUNT
    block = jnp.concatenate([g[:, :64], g[:, 64:]], axis=0)
    gram[...] = block
    t = lax.dot_general(
        factor[...], block, (((0,), (0,)), ((), ())), precision=lax.Precision.HIGHEST, preferred_element_type=jnp.float32
    )
    for r in range(32):
        term[r] = jnp.concatenate([t[r * 16 : r * 16 + 8], t[r * 16 + 8 : r * 16 + 16]], axis=1)


def close_body(parts, block, gram, out):
    gram[...] = block[...]
    v = jnp.sum(parts[...], axis=0)
    out[...] = jnp.concatenate([v[:, :64], v[:, 64:]], axis=0)


def swap(array, axes):
    return lax.all_to_all(array, axes, 0, 0, tiled=True)


def shards(pixels, factor):
    own = pixels.reshape(8, PLANES * OWN, LANES)
    rows = swap(twice(own), ("yo", "zl", "ya", "yb"))
    theirs = lax.ppermute(rows, "k", [(0, 1), (1, 0)])
    wide = pltpu.VMEM((1024, DEPTH), jnp.bfloat16)
    partial_gram = call(pair_body, f32(4, 4, 2, 64, LANES), (wide, wide), 2)(rows, theirs)
    partial_gram = swap(partial_gram.reshape(16, 128, LANES), ("x", "yb", "zl"))
    folded = call(fold_body, f32(4, 2, 16, LANES))(partial_gram.reshape(16, 2, 64, LANES))
    folded = swap(folded.reshape(8, 16, LANES), ("zh", "ya"))
    block, term = call(term_body, (f32(32, 64), f32(32, 8, LANES)), (), 2)(folded, factor)
    gram, projected = call(close_body, (result(32, 64), result(16, 64)), (), 2)(swap(term, ROW), block)
    return gram, projected.T


def solution(mesh):
    split = Mesh(mesh.devices.reshape(SIZES), AXES)
    in_specs = (P(None, None, ROW, COL), P(ROW, None))
    out_specs = (P(ROW, COL), P(COL, ROW))
    return jax.shard_map(shards, mesh=split, in_specs=in_specs, out_specs=out_specs, check_vma=False)
```

```python
import jax
import jax.numpy as jnp
from jax import lax
from jax.experimental import pallas as pl
from jax.experimental.pallas import tpu as pltpu
from jax.sharding import Mesh
from jax.sharding import PartitionSpec as P

AXES = ("zl", "yo", "ya", "yb", "k", "zh", "x")
SIZES = (2, 2, 2, 2, 2, 4, 4)
ROW = ("zl", "yo", "ya", "yb", "k")
COL = ("zh", "x")
PLANES, OWN, LANES = 3, 32, 128
DEPTH = PLANES * LANES
COUNT = 8 * 3 * 2048
NT = (((1,), (1,)), ((), ()))


def call(body, out, scratch=(), operands=1):
    vmem = pl.BlockSpec(memory_space=pltpu.VMEM)
    many = isinstance(out, tuple)
    kernel = pl.pallas_call(
        body,
        out_shape=out,
        in_specs=[vmem] * operands,
        out_specs=tuple(vmem for _ in out) if many else vmem,
        scratch_shapes=list(scratch),
    )
    return lambda *arrays: kernel(*(pltpu.with_memory_space_constraint(a, pltpu.VMEM) for a in arrays))


def f32(*shape):
    return pltpu.VMEM(shape, jnp.float32)


def result(*shape):
    return jax.ShapeDtypeStruct(shape, jnp.float32)


def split_rows(rows, high, low, first, stride):
    for x in range(4):
        for zl in range(2):
            for zh_lo in range(2):
                at = pl.multiple_of(first + (x * 4 + zl * 2 + zh_lo) * stride, 32)
                for p in range(PLANES):
                    v = rows[zh_lo * 8 + zl * 4 + x, p * OWN : (p + 1) * OWN, :]
                    h = v.astype(jnp.bfloat16)
                    high[pl.ds(at, OWN), p * LANES : (p + 1) * LANES] = h
                    low[pl.ds(at, OWN), p * LANES : (p + 1) * LANES] = (v - h.astype(jnp.float32)).astype(jnp.bfloat16)


def mine_body(mine, both):
    split_rows(mine, both.at[0], both.at[1], 0, 32)


def pair_body(theirs, mine, out, high, low):
    core = lax.axis_index("k")
    for block in range(16):
        at = pl.multiple_of(block * 64 + core * 32, 32)
        high[pl.ds(at, OWN), :] = mine[0, block * OWN : (block + 1) * OWN, :]
        low[pl.ds(at, OWN), :] = mine[1, block * OWN : (block + 1) * OWN, :]
    split_rows(theirs, high, low, (1 - core) * 32, 64)
    own = lax.axis_index("yo") * 64 + core * 32

    def own_rows(ref):
        order = [(ya * 2 + yb) * 256 + zl * 128 for yb in range(2) for zl in range(2) for ya in range(2)]
        return jnp.concatenate([ref[pl.ds(pl.multiple_of(own + at, 32), OWN), :] for at in order], axis=0)

    own_high, own_low = own_rows(high), own_rows(low)
    for x in range(4):
        h, l = high[x * 256 : (x + 1) * 256, :], low[x * 256 : (x + 1) * 256, :]
        g = lax.dot_general(own_high, l, NT, preferred_element_type=jnp.float32)
        g += lax.dot_general(own_low, h, NT, preferred_element_type=jnp.float32)
        g += lax.dot_general(own_high, h, NT, preferred_element_type=jnp.float32)
        for at in range(4):
            for zh in range(2):
                out[x, at, zh] = g[at * 64 : (at + 1) * 64, zh * LANES : (zh + 1) * LANES]


def fold_body(parts, out):
    left = lax.broadcasted_iota(jnp.int32, (16, LANES), 1) < 64
    for zh in range(2):
        for y in range(2):
            v = parts[0, zh, y * OWN : (y + 1) * OWN, :]
            for src in range(1, 16):
                v += parts[src, zh, y * OWN : (y + 1) * OWN, :]
            a, b = v[:16], v[16:]
            out[zh * 2, y] = jnp.where(left, a, pltpu.roll(b, 64, 1))
            out[zh * 2 + 1, y] = jnp.where(left, pltpu.roll(a, 64, 1), b)


def term_body(parts, factor, gram, term):
    g = jnp.sum(parts[...], axis=0) / COUNT
    block = jnp.concatenate([g[:, :64], g[:, 64:]], axis=0)
    gram[...] = block
    t = lax.dot_general(
        factor[...], block, (((0,), (0,)), ((), ())), precision=lax.Precision.HIGHEST, preferred_element_type=jnp.float32
    )
    for r in range(32):
        term[r] = jnp.concatenate([t[r * 16 : r * 16 + 8], t[r * 16 + 8 : r * 16 + 16]], axis=1)


def close_body(parts, block, gram, out):
    gram[...] = block[...]
    v = jnp.sum(parts[...], axis=0)
    out[...] = jnp.concatenate([v[:, :64], v[:, 64:]], axis=0)


def swap(array, axes):
    return lax.all_to_all(array, axes, 0, 0, tiled=True)


def shards(pixels, factor):
    own = pixels.reshape(8, PLANES * OWN, LANES)
    rows = swap(jnp.concatenate([own, own]), ("yo", "zl", "ya", "yb"))
    theirs = lax.ppermute(rows, "k", [(0, 1), (1, 0)])
    wide = pltpu.VMEM((1024, DEPTH), jnp.bfloat16)
    mine = call(mine_body, pltpu.VMEM((2, 512, DEPTH), jnp.bfloat16))(rows)
    partial_gram = call(pair_body, f32(4, 4, 2, 64, LANES), (wide, wide), 2)(theirs, mine)
    partial_gram = swap(partial_gram.reshape(16, 128, LANES), ("x", "yb", "zl"))
    folded = call(fold_body, f32(4, 2, 16, LANES))(partial_gram.reshape(16, 2, 64, LANES))
    folded = swap(folded.reshape(8, 16, LANES), ("zh", "ya"))
    block, term = call(term_body, (f32(32, 64), f32(32, 8, LANES)), (), 2)(folded, factor)
    gram, projected = call(close_body, (result(32, 64), result(16, 64)), (), 2)(swap(term, ROW), block)
    return gram, projected.T


def solution(mesh):
    split = Mesh(mesh.devices.reshape(SIZES), AXES)
    in_specs = (P(None, None, ROW, COL), P(ROW, None))
    out_specs = (P(ROW, COL), P(COL, ROW))
    return jax.shard_map(shards, mesh=split, in_specs=in_specs, out_specs=out_specs, check_vma=False)
```
